128 devices in a mesh: seq: 32 (over y, z_hi, x), sub: 4 (over z_lo, core).
Axes of the slice: x: 4, y: 4, z: 4 (z_hi: 2, z_lo: 2; z = z_hi * 2 + z_lo), core: 2. Of those that a mesh axis runs over, the one named last changes fastest.
Arguments:
- tokens: bfloat16 [8192, 4096], P('seq'), may hold values from -6 to 6
- w_split: bfloat16 [4096, 4096], P(None, 'sub'), may hold values from -0.09375 to 0.09375
- w_merge: bfloat16 [4096, 4096], P('sub'), may hold values from -0.09375 to 0.09375
- expert_in: bfloat16 [128, 1024, 2048], P(('seq', 'sub')), may hold values from -0.1875 to 0.1875
- expert_out: bfloat16 [128, 1024, 1024], P(('seq', 'sub')), may hold values from -0.1875 to 0.1875
- expert_ids: int32 [4, 8192, 2], P('sub', 'seq'), may hold values from 0 to 127, all different within a row; in each aligned block of 256 rows (0 to 255, 256 to 511, ..., all dimensions but the last counted through in order) at most 6 rows name the same one
- combine_q: int32 [4, 8192, 2], P('sub', 'seq'), may hold values from 4096 to 65536
- capacity: int32 [128], replicated, may hold values from 3 to 6
Outputs:
- mixed: bfloat16 [8192, 4096], P('seq', 'sub')
The draws below stay inside these ranges and needn't reach their ends.
Inputs may be any that keep to these rules, and one draw needn't show every extreme that they name: `expert_ids`: in each block of 256 positions of one sub-head, the ids of a position differ, no expert is named more than 6 times, a bound that some block reaches.
All inputs are finite; a program needn't handle non-finite values.
Results may differ from the reference program's by a relative error of at most 0.0076.
Values may be sent and summed in bfloat16 or wider, within the bound.
A program may use at most 128 MiB of HBM per device.

```python
import math
import jax
import jax.numpy as jnp
import numpy as np
from jax import lax

D = 4096
HEADS = 4
FFE = 1024
TOPK = 2
TOK_DEV = 256
SUBW = 1024
EXPERTS = 128
CAP = 6
TOKENS = 8192
N_SEQ = 32


def with_ends(entries, rng, smallest, high):
    longest = entries.shape.index(max(entries.shape))
    spots = []
    for shift in (0, 1):
        where = [jax.random.randint(jax.random.fold_in(rng, axis), (), 0, length) for axis, length in enumerate(entries.shape)]
        where[longest] = (where[longest] + shift) % entries.shape[longest]
        spots.append(tuple(where))
    return entries.at[spots[0]].set(smallest).at[spots[1]].set(high)


def shard_levels(key, extent, split, least, top_value):
    def one(axis_at, blocks):
        draws = jax.random.uniform(jax.random.fold_in(jax.random.fold_in(key, 6), axis_at), (blocks,), jnp.float32, least / len(split), top_value / len(split))
        return jnp.repeat(jnp.exp(draws), extent[axis_at] // blocks).reshape((-1,) + (1,) * (len(extent) - axis_at - 1))

    gain = one(*split[0])
    for cut in split[1:]:
        gain = gain * one(*cut)
    return gain


def deal_out(rng, own, number, rows, number_of, top, limit, lean):
    ranking = jax.random.permutation(rng, number_of)
    crowded, common = shares(number_of, rows * top, limit, lean, True), shares(number_of, rows * top, limit, lean, False)
    places = jnp.arange(number_of)

    def named(lengths, rotation):
        used = int((lengths > 0).sum())
        fixed = max(1, used // 4)
        moved = fixed + (places - fixed + rotation * (used - fixed)) % max(1, number_of - fixed)
        return jnp.zeros((number_of,), jnp.int32).at[ranking[jnp.where(places < fixed, places, moved)]].set(jnp.asarray(lengths, jnp.int32))

    lengths = jnp.where(number % 4 == 0, named(crowded, number // 4), named(common, number - number // 4 - 1))
    mixed = jax.random.permutation(jax.random.fold_in(own, 3), number_of)
    source_of, sink = mixed[0:number_of // 2 * 2:2], mixed[1:number_of // 2 * 2:2]
    slack = jnp.minimum(lengths[source_of] - 1, limit - lengths[sink]) // 2
    slack = jnp.where((source_of == ranking[0]) | (sink == ranking[0]) | (lengths[sink] == 0), 0, jnp.maximum(slack, 0))
    moved = jax.random.randint(jax.random.fold_in(own, 4), (number_of // 2,), 0, 1 << 20) % (slack + 1)
    lengths = lengths.at[source_of].add(-moved).at[sink].add(moved)
    members = jnp.searchsorted(jnp.cumsum(lengths), jnp.arange(rows * top), side="right").astype(jnp.int32)
    table = members.reshape(top, rows).T
    table = table[jax.random.permutation(jax.random.fold_in(own, 1), rows)]
    rotation = jax.random.randint(jax.random.fold_in(own, 2), (rows, 1), 0, top)
    return jnp.take_along_axis(table, (jnp.arange(top)[None, :] + rotation) % top, axis=1)


def shares(number_of, total, limit, slope, full):
    loads = [(1 << 20) // math.isqrt(rank ** slope) + 1 for rank in range(1, number_of + 1)]
    largest = limit if full else min(limit, max(-(-total // number_of), total * loads[0] // sum(loads)))
    least = 1 if total - largest >= number_of - 1 else 0
    counts, rest = [largest] + [least] * (number_of - 1), total - largest - least * (number_of - 1)
    while rest > 0:
        candidates = [i for i in range(1, number_of) if counts[i] < largest] or [i for i in range(1, number_of) if counts[i] < limit]
        mass, remaining = sum([loads[i] for i in candidates]), rest
        for i in candidates:
            addition = min(limit - counts[i], max(1, remaining * loads[i] // mass), rest)
            counts[i] = counts[i] + addition
            rest = rest - addition
    return np.array(counts)


def centred(key, shape, scale, bound, split=(), kind=jnp.bfloat16):
    array = scale * jax.random.normal(key, shape, jnp.float32)
    if split:
        array = array * shard_levels(key, shape, split, -0.22, 0.18)
    return jnp.clip(array, -bound, bound).astype(kind)


def setup_inputs(seed: int = 0) -> dict:
    key_of = jax.random.split(jax.random.key(seed), 9)
    tokens = centred(key_of[0], (TOKENS, D), 1.0, 6.0, ((0, 32),))
    w_split = centred(key_of[1], (D, D), D ** -0.5, 0.09375, ((1, 4),))
    w_merge = centred(key_of[2], (D, D), D ** -0.5, 0.09375, ((0, 4),))
    expert_in = centred(key_of[3], (EXPERTS, SUBW, 2 * FFE), SUBW ** -0.5, 0.1875, ((0, 128),))
    expert_out = centred(key_of[4], (EXPERTS, FFE, SUBW), FFE ** -0.5, 0.1875, ((0, 128),))
    expert_ids_keys = jax.random.split(jax.random.fold_in(key_of[5], 1), HEADS * TOKENS // TOK_DEV)
    expert_ids_turns = jax.random.permutation(jax.random.fold_in(key_of[5], 3), HEADS * TOKENS // TOK_DEV)
    expert_ids = jax.vmap(lambda own, number: deal_out(jax.random.fold_in(key_of[5], 2), own, number, TOK_DEV, EXPERTS, TOPK, CAP, 2))(expert_ids_keys, expert_ids_turns).reshape((HEADS, TOKENS, TOPK))
    combine_q = with_ends(jax.random.randint(key_of[6], (HEADS, TOKENS, TOPK), 4096, 65537), jax.random.fold_in(key_of[6], 1), 4096, 65536).astype(jnp.int32)
    capacity = with_ends(jax.random.randint(key_of[7], (EXPERTS,), CAP // 2, CAP + 1), jax.random.fold_in(key_of[7], 1), CAP // 2, CAP).astype(jnp.int32)
    return {"tokens": tokens, "w_split": w_split, "w_merge": w_merge, "expert_in": expert_in, "expert_out": expert_out, "expert_ids": expert_ids, "combine_q": combine_q, "capacity": capacity}


def expert_ffn(inputs, w_in, w_out):
    gate_up = jnp.dot(inputs, w_in, preferred_element_type=jnp.float32)
    ffe_width = w_out.shape[0]
    hidden = (jax.nn.silu(gate_up[:, :ffe_width]) * gate_up[:, ffe_width:]).astype(jnp.bfloat16)
    return jnp.dot(hidden, w_out, preferred_element_type=jnp.float32).astype(jnp.bfloat16)


def reference(tokens, w_split, w_merge, expert_in, expert_out, expert_ids, combine_q, capacity):
    sub_tokens = jnp.dot(tokens, w_split, preferred_element_type=jnp.float32).astype(jnp.bfloat16)
    table = sub_tokens.reshape(TOKENS, HEADS, SUBW).transpose(1, 0, 2).reshape(HEADS * TOKENS, SUBW)
    block_count = HEADS * N_SEQ
    expert_of = expert_ids.reshape(block_count, TOPK * TOK_DEV)
    onehot = (expert_of[:, :, None] == jnp.arange(EXPERTS, dtype=jnp.int32)[None, None, :]).astype(jnp.int32)
    order_rank = jnp.sum((jnp.cumsum(onehot, axis=1) - onehot) * onehot, axis=2)
    cap_limit = jnp.sum(onehot * capacity[None, None, :], axis=2)
    is_kept = order_rank < cap_limit
    block_id = jnp.arange(block_count, dtype=jnp.int32)[:, None]
    slot_index = (expert_of * block_count + block_id) * CAP + order_rank
    total_slots = EXPERTS * block_count * CAP
    slot_index = jnp.where(is_kept, slot_index, total_slots)
    entry_pos = jnp.arange(TOPK * TOK_DEV, dtype=jnp.int32)[None, :]
    row_index = block_id * TOK_DEV + entry_pos // TOPK
    weights = combine_q.reshape(block_count, TOPK * TOK_DEV).astype(jnp.float32) / 65536.0
    slot_row = jnp.full((total_slots,), -1, jnp.int32).at[slot_index.reshape(-1)].set(
        jnp.broadcast_to(row_index, slot_index.shape).reshape(-1), mode="drop")
    slot_weight = jnp.zeros((total_slots,), jnp.float32).at[slot_index.reshape(-1)].set(
        weights.reshape(-1), mode="drop")
    slot_row = slot_row.reshape(EXPERTS, block_count * CAP)
    slot_weight = slot_weight.reshape(EXPERTS, block_count * CAP)

    def one_expert(running, inputs_e):
        rows_here, weights_here, w_in, w_out = inputs_e
        is_valid = rows_here >= 0
        safe_row = jnp.maximum(rows_here, 0)
        picked = jnp.where(is_valid[:, None], table[safe_row], jnp.zeros((), jnp.bfloat16))
        answer = expert_ffn(picked, w_in, w_out)
        weighted = jnp.where(is_valid[:, None], weights_here[:, None] * answer.astype(jnp.float32), jnp.zeros((), jnp.float32))
        return running.at[safe_row].add(weighted), None

    start = jnp.zeros((HEADS * TOKENS, SUBW), jnp.float32)
    running, _ = lax.scan(one_expert, start, (slot_row, slot_weight, expert_in, expert_out))
    head_out = running.astype(jnp.bfloat16).reshape(HEADS, TOKENS, SUBW).transpose(1, 0, 2).reshape(TOKENS, D)
    return jnp.dot(head_out, w_merge, preferred_element_type=jnp.float32).astype(jnp.bfloat16)
```

```python
import jax
import jax.numpy as jnp
from jax import lax
from jax.experimental import pallas as pl
from jax.experimental.pallas import tpu as pltpu
from jax.sharding import PartitionSpec as P

MESH = pl.DeviceIdType.MESH
PEERS = 128
MUL = 45
INV = 37
PARTS = 4
PER = PEERS // PARTS
SLOTS = 6
PAD = 8


def my_coords():
    s = lax.axis_index("seq")
    u = lax.axis_index("sub")
    return s % 4, s // 8, ((s // 4) % 2) * 2 + u // 2, u % 2


def device_at(x, y, z, c):
    return (y * 8 + (z // 2) * 4 + x, (z % 2) * 2 + c)


def peer(me, i, sign):
    r = (i * MUL) % PEERS
    dc = r % 2
    dx = (r // 2) % 4
    dz = (r // 8) % 4
    dy = r // 32
    x, y, z, c = me
    if sign < 0:
        dx, dz, dy = 4 - dx, 4 - dz, 4 - dy
    return device_at((x + dx) % 4, (y + dy) % 4, (z + dz) % 4, (c + dc) % 2)


def dot(a, b):
    return jnp.dot(a, b, preferred_element_type=jnp.float32)


def kernel(
    ids, quota, cap, tokens_h, ws_h, wm_h, win_h, wout_h,
    out,
    tokens, ws, wm, win, wout, sub_tok, chosen, comb, packed, recv, act, ans, ret, head, headb,
    dd_s, dd_r, z_s, z_r, f_s, f_r, keep,
    ld_sem, wm_sem, ds_sem, dr_sem, rs_sem, rr_sem, dd_ss, dd_rs, z_ss, z_rs, f_ss, f_rs,
):
    me = my_coords()
    mx, my, mz, mc = me
    zl = mz % 2
    barrier = pltpu.get_barrier_semaphore()

    loads = [pltpu.make_async_copy(tokens_h, tokens, ld_sem.at[0])]
    for n in range(4):
        loads.append(pltpu.make_async_copy(ws_h.at[:, pl.ds(n * 256, 256)], ws.at[n], ld_sem.at[1 + n]))
    loads.append(pltpu.make_async_copy(win_h, win, ld_sem.at[5]))
    loads.append(pltpu.make_async_copy(wout_h, wout, ld_sem.at[6]))
    quarters = [
        (1 - zl) * 2 + (1 - mc),
        (1 - zl) * 2 + mc,
        zl * 2 + (1 - mc),
        zl * 2 + mc,
    ]
    for n in range(4):
        col = pl.multiple_of(quarters[n] * 1024, 1024)
        loads.append(pltpu.make_async_copy(wm_h.at[:, pl.ds(col, 1024)], wm.at[n], wm_sem.at[n]))
    for cp in loads:
        cp.start()

    def clear(i, carry):
        ret[pl.ds(i * 8, 8)] = jnp.zeros((8, PAD, 1024), jnp.bfloat16)
        return carry

    lax.fori_loop(0, 16, clear, 0)

    def greet(i, carry):
        pl.semaphore_signal(barrier, inc=1, device_id=peer(me, i, 1), device_id_type=MESH)
        return carry

    lax.fori_loop(1, PEERS, greet, 0)

    e = lax.broadcasted_iota(jnp.int32, (128, 256), 0)
    id0 = ids[0:1, :]
    id1 = ids[1:2, :]
    oh0 = (e == id0).astype(jnp.float32)
    oh1 = (e == id1).astype(jnp.float32)
    tri = (
        lax.broadcasted_iota(jnp.int32, (256, 256), 0) < lax.broadcasted_iota(jnp.int32, (256, 256), 1)
    ).astype(jnp.bfloat16)
    before = dot((oh0 + oh1).astype(jnp.bfloat16), tri)
    rank0 = jnp.sum(oh0 * before, axis=0, keepdims=True)
    rank1 = jnp.sum(oh1 * before, axis=0, keepdims=True)
    sq0 = lax.broadcasted_iota(jnp.int32, (128, 128), 0)
    sq1 = lax.broadcasted_iota(jnp.int32, (128, 128), 1)
    cap_col = jnp.sum(jnp.where(sq0 == sq1, cap[0:1, :].astype(jnp.float32), 0.0), axis=1, keepdims=True)
    lim0 = jnp.sum(oh0 * cap_col, axis=0, keepdims=True)
    lim1 = jnp.sum(oh1 * cap_col, axis=0, keepdims=True)

    def place(ident):
        ec = ident & 1
        ex = (ident >> 2) & 3
        ez = ((ident >> 4) & 1) * 2 + ((ident >> 1) & 1)
        ey = ident >> 5
        r = (((ey - my) & 3) << 5) + (((ez - mz) & 3) << 3) + (((ex - mx) & 3) << 1) + ((ec - mc) & 1)
        return ((r * INV) & (PEERS - 1)) * PAD

    loc0 = place(id0) + rank0.astype(jnp.int32)
    loc1 = place(id1) + rank1.astype(jnp.int32)
    w0 = jnp.where(rank0 < lim0, quota[0:1, :].astype(jnp.float32) * (1.0 / 65536.0), 0.0)
    w1 = jnp.where(rank1 < lim1, quota[1:2, :].astype(jnp.float32) * (1.0 / 65536.0), 0.0)

    for j in range(4):
        p = lax.broadcasted_iota(jnp.int32, (256, 256), 0) + j * 256
        hit = jnp.logical_or(p == loc0, p == loc1)
        chosen[pl.ds(j * 256, 256)] = jnp.where(hit, 1.0, 0.0).astype(jnp.bfloat16)
    rows = jnp.concatenate(
        [loc0.astype(jnp.float32), loc1.astype(jnp.float32), w0, w1, jnp.zeros((4, 256), jnp.float32)], axis=0
    )
    cols = rows.T
    l0 = cols[:, 0:1]
    l1 = cols[:, 1:2]
    v0 = cols[:, 2:3]
    v1 = cols[:, 3:4]
    for j in range(4):
        p = (lax.broadcasted_iota(jnp.int32, (256, 256), 1) + j * 256).astype(jnp.float32)
        c = jnp.where(p == l0, v0, jnp.where(p == l1, v1, 0.0))
        comb[j] = c.astype(jnp.bfloat16)

    loads[0].wait()
    for n in range(4):
        loads[1 + n].wait()
        sub_tok[:, pl.ds(n * 256, 256)] = dot(tokens[...], ws[n]).astype(jnp.bfloat16)

    for j in range(PARTS):
        rows_j = dot(chosen[pl.ds(j * 256, 256)], sub_tok[...]).astype(jnp.bfloat16)
        packed[pl.ds(j * PER, PER)] = rows_j.reshape(PER, PAD, 1024)

    pl.semaphore_wait(barrier, PEERS - 1)

    def six(ref, i):
        return ref.at[i, pl.ds(0, SLOTS)]

    def six_many(ref, i, n):
        return ref.at[pl.ds(i, n), pl.ds(0, SLOTS)]

    def dispatch(i, carry):
        pltpu.make_async_remote_copy(
            src_ref=six(packed, i), dst_ref=six(recv, i),
            send_sem=ds_sem, recv_sem=dr_sem.at[i // PER],
            device_id=peer(me, i, 1), device_id_type=MESH,
        ).start()
        return carry

    lax.fori_loop(1, PEERS, dispatch, 0)
    recv[0] = packed[0]

    loads[5].wait()
    loads[6].wait()

    def landed(ref, sem, j):
        if j == 0:
            return pltpu.make_async_copy(six_many(ref, 1, PER - 1), six_many(ref, 1, PER - 1), sem.at[0])
        return pltpu.make_async_copy(six_many(ref, j * PER, PER), six_many(ref, j * PER, PER), sem.at[j])

    for j in range(PARTS):
        landed(recv, dr_sem, j).wait()
        x = recv[pl.ds(j * PER, PER)].reshape(PER * PAD, 1024)
        for n in range(4):
            g = dot(x, win[:, pl.ds(n * 256, 256)])
            u = dot(x, win[:, pl.ds(1024 + n * 256, 256)])
            act[:, pl.ds(n * 256, 256)] = (g / (1.0 + jnp.exp(-g)) * u).astype(jnp.bfloat16)
        for n in range(4):
            r = dot(act[...], wout[:, pl.ds(n * 256, 256)]).astype(jnp.bfloat16)
            ans[pl.ds(j * PER, PER), :, pl.ds(n * 256, 256)] = r.reshape(PER, PAD, 256)

        def give_back(i, carry):
            pltpu.make_async_remote_copy(
                src_ref=six(ans, i), dst_ref=six(ret, i),
                send_sem=rs_sem, recv_sem=rr_sem.at[j],
                device_id=peer(me, i, -1), device_id_type=MESH,
            ).start()
            return carry

        lax.fori_loop(max(1, j * PER), (j + 1) * PER, give_back, 0)
        if j == 0:
            ret[0] = ans[0]

    for j in range(PARTS):
        landed(ret, rr_sem, j).wait()
        part = dot(comb[j], ret[pl.ds(j * PER, PER)].reshape(PER * PAD, 1024))
        if j == 0:
            head[...] = part
        elif j < PARTS - 1:
            head[...] += part
        else:
            headb[...] = (head[...] + part).astype(jnp.bfloat16)

    for n in range(4):
        loads[7 + n].wait()

    partner = device_at(mx, my, mz, 1 - mc)
    across = device_at(mx, my, mz + 1 - 2 * zl, mc)

    def send(src, dst, ss, rs, b, to):
        return pltpu.make_async_remote_copy(
            src_ref=src.at[b], dst_ref=dst.at[b], send_sem=ss.at[b], recv_sem=rs.at[b],
            device_id=to, device_id_type=MESH,
        )

    def product(n, b):
        return dot(headb[...], wm[n, :, pl.ds(b * 256, 256)])

    def first(b):
        dd_s[b] = product(0, b).astype(jnp.bfloat16)
        send(dd_s, dd_r, dd_ss, dd_rs, b, partner).start()

    def second(b):
        mine = product(1, b)
        send(dd_s, dd_r, dd_ss, dd_rs, b, partner).wait_recv()
        z_s[b] = (mine + dd_r[b].astype(jnp.float32)).astype(jnp.bfloat16)
        send(z_s, z_r, z_ss, z_rs, b, across).start()

    first(0)
    first(1)
    second(0)
    first(2)
    second(1)
    first(3)
    second(2)
    second(3)
    for b in range(4):
        f_s[b] = product(2, b).astype(jnp.bfloat16)
        send(f_s, f_r, f_ss, f_rs, b, partner).start()
    for b in range(4):
        keep[b] = product(3, b)
    for b in range(4):
        send(f_s, f_r, f_ss, f_rs, b, partner).wait_recv()
        keep[b] += f_r[b].astype(jnp.float32)
    for b in range(4):
        send(z_s, z_r, z_ss, z_rs, b, across).wait_recv()
        out[:, pl.ds(b * 256, 256)] = (keep[b] + z_r[b].astype(jnp.float32)).astype(jnp.bfloat16)

    pltpu.make_async_copy(six_many(packed, 1, PEERS - 1), six_many(packed, 1, PEERS - 1), ds_sem).wait()
    pltpu.make_async_copy(six_many(ans, 1, PEERS - 1), six_many(ans, 1, PEERS - 1), rs_sem).wait()
    for b in range(4):
        send(dd_s, dd_r, dd_ss, dd_rs, b, partner).wait_send()
        send(z_s, z_r, z_ss, z_rs, b, across).wait_send()
        send(f_s, f_r, f_ss, f_rs, b, partner).wait_send()


def body(tokens, w_split, w_merge, expert_in, expert_out, expert_ids, combine_q, capacity):
    bf, f32 = jnp.bfloat16, jnp.float32
    vmem = pl.BlockSpec(memory_space=pltpu.VMEM)
    hbm = pl.BlockSpec(memory_space=pl.ANY)
    dma = pltpu.SemaphoreType.DMA
    quarter = pltpu.VMEM((4, 256, 256), bf)
    return pl.pallas_call(
        kernel,
        out_shape=jax.ShapeDtypeStruct((256, 1024), bf),
        in_specs=[vmem] * 3 + [hbm] * 5,
        out_specs=vmem,
        scratch_shapes=[
            pltpu.VMEM((256, 4096), bf),
            pltpu.VMEM((4, 4096, 256), bf),
            pltpu.VMEM((4, 1024, 1024), bf),
            pltpu.VMEM((1024, 2048), bf),
            pltpu.VMEM((1024, 1024), bf),
            pltpu.VMEM((256, 1024), bf),
            pltpu.VMEM((1024, 256), bf),
            pltpu.VMEM((4, 256, 256), bf),
            pltpu.VMEM((PEERS, PAD, 1024), bf),
            pltpu.VMEM((PEERS, PAD, 1024), bf),
            pltpu.VMEM((PER * PAD, 1024), bf),
            pltpu.VMEM((PEERS, PAD, 1024), bf),
            pltpu.VMEM((PEERS, PAD, 1024), bf),
            pltpu.VMEM((256, 1024), f32),
            pltpu.VMEM((256, 1024), bf),
            quarter, quarter, quarter, quarter, quarter, quarter,
            pltpu.VMEM((4, 256, 256), f32),
            dma((7,)), dma((4,)), dma, dma((PARTS,)), dma, dma((PARTS,)),
            dma((4,)), dma((4,)), dma((4,)), dma((4,)), dma((4,)), dma((4,)),
        ],
        compiler_params=pltpu.CompilerParams(
            collective_id=0, has_side_effects=True, vmem_limit_bytes=58 * 2**20
        ),
    )(
        expert_ids[0].T,
        combine_q[0].T,
        capacity.reshape(1, -1),
        tokens,
        w_split,
        w_merge,
        expert_in[0],
        expert_out[0],
    )


def solution(mesh):
    in_specs = (
        P("seq", None),
        P(None, "sub"),
        P("sub", None),
        P(("seq", "sub"), None, None),
        P(("seq", "sub"), None, None),
        P("sub", "seq", None),
        P("sub", "seq", None),
        P(),
    )
    return jax.shard_map(body, mesh=mesh, in_specs=in_specs, out_specs=P("seq", "sub"), check_vma=False)
```

```python
import jax
import jax.numpy as jnp
import numpy as np
from jax import lax
from jax.experimental import pallas as pl
from jax.experimental.pallas import tpu as pltpu
from jax.sharding import PartitionSpec as P

MESH = pl.DeviceIdType.MESH
PEERS = 128
SLOTS = 6
PAD = 8
EDGES = (0, 32, 64, 96, 128)
EARLY = 40
MUL = 45
PARTS = len(EDGES) - 1


def step_of(r):
    return (r // 2) % 4, r // 32, (r // 8) % 4, r % 2


def hops(r):
    return sum((0, 1, 2, 1)[d] for d in step_of(r)[:3])


def mixed():
    return [(i * MUL) % PEERS for i in range(1, PEERS)] + [0]


ORDER = mixed()
POSITION = np.argsort(np.array(ORDER)).astype(np.int32)


def part_of(i):
    return max(j for j in range(PARTS) if EDGES[j] <= i)


def dot(a, b):
    return jnp.dot(a, b, preferred_element_type=jnp.float32)


def kernel(
    ids_h, quota_h, cap_h, table_h, tokens_h, ws_h, wm_h, win_h, wout_h,
    keep, z_r,
    ids, quota, cap, table,
    tokens, ws, wm, win, wout, sub_tok, chosen, comb, packed, recv, act, ans, ret, head, headb,
    dd_s, dd_r, z_s, f_s, f_r,
    sm_sem, ld_sem, wm_sem, ds_sem, dr_sem, rs_sem, rr_sem, dd_ss, dd_rs, z_ss, z_rs, f_ss, f_rs,
):
    s = lax.axis_index("seq")
    u = lax.axis_index("sub")
    mx, my, mz, mc = s % 4, s // 8, ((s // 4) % 2) * 2 + u // 2, u % 2
    zl = mz % 2
    xs = [(mx + d) % 4 for d in range(4)]
    ys = [((my + d) % 4) * 8 for d in range(4)]
    zs = [(mz + d) % 4 for d in range(4)]
    zh = [(z // 2) * 4 for z in zs]
    zw = [(z % 2) * 2 for z in zs]
    cs = [(mc + d) % 2 for d in range(2)]

    def peer(i, sign=1):
        dx, dy, dz, dc = step_of(ORDER[i])
        if sign < 0:
            dx, dy, dz = -dx % 4, -dy % 4, -dz % 4
        return (ys[dy] + zh[dz] + xs[dx], zw[dz] + cs[dc])

    barrier = pltpu.get_barrier_semaphore()

    loads = [pltpu.make_async_copy(tokens_h, tokens, ld_sem.at[0])]
    for n in range(2):
        loads.append(pltpu.make_async_copy(ws_h.at[:, pl.ds(n * 512, 512)], ws.at[n], ld_sem.at[1 + n]))
    small = [
        pltpu.make_async_copy(ids_h, ids, sm_sem.at[0]),
        pltpu.make_async_copy(quota_h, quota, sm_sem.at[1]),
        pltpu.make_async_copy(cap_h, cap, sm_sem.at[2]),
        pltpu.make_async_copy(table_h, table, sm_sem.at[3]),
    ]
    for cp in small + loads:
        cp.start()
    for i in sorted(range(PEERS - 1), key=lambda i: -hops(ORDER[i])):
        pl.semaphore_signal(barrier, inc=1, device_id=peer(i), device_id_type=MESH)

    loads.append(pltpu.make_async_copy(win_h, win, ld_sem.at[3]))
    loads.append(pltpu.make_async_copy(wout_h, wout, ld_sem.at[4]))
    quarters = [
        (1 - zl) * 2 + (1 - mc),
        (1 - zl) * 2 + mc,
        zl * 2 + (1 - mc),
        zl * 2 + mc,
    ]
    for n in range(4):
        col = pl.multiple_of(quarters[n] * 1024, 1024)
        loads.append(pltpu.make_async_copy(wm_h.at[:, pl.ds(col, 1024)], wm.at[n], wm_sem.at[n]))

    def clear(i, carry):
        ret[pl.ds(i * 8, 8)] = jnp.zeros((8, PAD, 1024), jnp.bfloat16)
        return carry

    lax.fori_loop(0, 16, clear, 0)

    with jax.named_scope("small"):
        for cp in small:
            cp.wait()
    with jax.named_scope("route"):
        e = lax.broadcasted_iota(jnp.int32, (128, 256), 0)
        id0 = ids[0:1, :]
        id1 = ids[1:2, :]
        oh0 = (e == id0).astype(jnp.float32)
        oh1 = (e == id1).astype(jnp.float32)
        tri = (
            lax.broadcasted_iota(jnp.int32, (256, 256), 0) < lax.broadcasted_iota(jnp.int32, (256, 256), 1)
        ).astype(jnp.bfloat16)
        before = dot((oh0 + oh1).astype(jnp.bfloat16), tri)
        rank0 = jnp.sum(oh0 * before, axis=0, keepdims=True)
        rank1 = jnp.sum(oh1 * before, axis=0, keepdims=True)
        sq0 = lax.broadcasted_iota(jnp.int32, (128, 128), 0)
        sq1 = lax.broadcasted_iota(jnp.int32, (128, 128), 1)
        cap_col = jnp.sum(jnp.where(sq0 == sq1, cap[0:1, :].astype(jnp.float32), 0.0), axis=1, keepdims=True)
        ec = sq0 & 1
        ex = (sq0 >> 2) & 3
        ez = ((sq0 >> 4) & 1) * 2 + ((sq0 >> 1) & 1)
        ey = sq0 >> 5
        r = (((ey - my) & 3) << 5) + (((ez - mz) & 3) << 3) + (((ex - mx) & 3) << 1) + ((ec - mc) & 1)
        pos_col = jnp.sum(jnp.where(r == sq1, table[0:1, :].astype(jnp.float32), 0.0), axis=1, keepdims=True)
        lim0 = jnp.sum(oh0 * cap_col, axis=0, keepdims=True)
        lim1 = jnp.sum(oh1 * cap_col, axis=0, keepdims=True)
        loc0 = jnp.sum(oh0 * pos_col, axis=0, keepdims=True) * PAD + rank0
        loc1 = jnp.sum(oh1 * pos_col, axis=0, keepdims=True) * PAD + rank1
        w0 = jnp.where(rank0 < lim0, quota[0:1, :].astype(jnp.float32) * (1.0 / 65536.0), 0.0)
        w1 = jnp.where(rank1 < lim1, quota[1:2, :].astype(jnp.float32) * (1.0 / 65536.0), 0.0)

        for j in range(4):
            p = (lax.broadcasted_iota(jnp.int32, (256, 256), 0) + j * 256).astype(jnp.float32)
            hit = jnp.logical_or(p == loc0, p == loc1)
            chosen[pl.ds(j * 256, 256)] = jnp.where(hit, 1.0, 0.0).astype(jnp.bfloat16)

    def six(ref, i, half):
        return ref.at[i, pl.ds(0, SLOTS), pl.ds(half * 512, 512)]

    def row(ref, i):
        return ref.at[i, pl.ds(0, SLOTS)]

    def rows(ref, i, n):
        return ref.at[pl.ds(i, n), pl.ds(0, SLOTS)]

    def out_to(src, dst, i):
        pltpu.make_async_remote_copy(
            src_ref=src, dst_ref=dst, send_sem=ds_sem, recv_sem=dr_sem.at[part_of(i)],
            device_id=peer(i), device_id_type=MESH,
        ).start()

    loads[0].wait()
    for half in range(2):
        with jax.named_scope(f"split{half}"):
            loads[1 + half].wait()
            cols = pl.ds(half * 512, 512)
            sub_tok[:, cols] = dot(tokens[...], ws[half]).astype(jnp.bfloat16)
        with jax.named_scope(f"pack{half}"):
            if half == 1:
                for cp in loads[3:]:
                    cp.start()
            for j in range(4):
                rows_j = dot(chosen[pl.ds(j * 256, 256)], sub_tok[:, cols]).astype(jnp.bfloat16)
                packed[pl.ds(j * 32, 32), :, cols] = rows_j.reshape(32, PAD, 512)
        with jax.named_scope(f"send{half}"):
            if half == 0:
                pl.semaphore_wait(barrier, PEERS - 1)
            for i in range(EARLY):
                out_to(six(packed, i, half), six(recv, i, half), i)
    with jax.named_scope("send_rest"):
        for i in range(EARLY, PEERS - 1):
            out_to(row(packed, i), row(recv, i), i)
    recv[PEERS - 1] = packed[PEERS - 1]

    with jax.named_scope("comb"):
        stacked = jnp.concatenate([loc0, loc1, w0, w1, jnp.zeros((4, 256), jnp.float32)], axis=0)
        turned = stacked.T
        l0 = turned[:, 0:1]
        l1 = turned[:, 1:2]
        v0 = turned[:, 2:3]
        v1 = turned[:, 3:4]
        for j in range(4):
            p = (lax.broadcasted_iota(jnp.int32, (256, 256), 1) + j * 256).astype(jnp.float32)
            c = jnp.where(p == l0, v0, jnp.where(p == l1, v1, 0.0))
            comb[:, pl.ds(j * 256, 256)] = c.astype(jnp.bfloat16)

    loads[3].wait()
    loads[4].wait()

    def landed(ref, sem, j):
        lo, hi = EDGES[j], min(EDGES[j + 1], PEERS - 1)
        return pltpu.make_async_copy(rows(ref, lo, hi - lo), rows(ref, lo, hi - lo), sem.at[j])

    def give_back(j):
        with jax.named_scope(f"back{j}"):
            for i in range(EDGES[j], min(EDGES[j + 1], PEERS - 1)):
                pltpu.make_async_remote_copy(
                    src_ref=row(ans, i), dst_ref=row(ret, i),
                    send_sem=rs_sem, recv_sem=rr_sem.at[j],
                    device_id=peer(i, -1), device_id_type=MESH,
                ).start()

    for j in range(PARTS):
        lo, n_rows = EDGES[j], (EDGES[j + 1] - EDGES[j]) * PAD
        with jax.named_scope(f"wait{j}"):
            landed(recv, dr_sem, j).wait()
        with jax.named_scope(f"ffn{j}"):
            x = recv[pl.ds(lo, n_rows // PAD)].reshape(n_rows, 1024)
            for n in range(4):
                g = dot(x, win[:, pl.ds(n * 256, 256)])
                t = dot(x, win[:, pl.ds(1024 + n * 256, 256)])
                act[pl.ds(0, n_rows), pl.ds(n * 256, 256)] = (g / (1.0 + jnp.exp(-g)) * t).astype(jnp.bfloat16)
            for n in range(2):
                a = dot(act[pl.ds(0, n_rows)], wout[:, pl.ds(n * 512, 512)]).astype(jnp.bfloat16)
                ans[pl.ds(lo, n_rows // PAD), :, pl.ds(n * 512, 512)] = a.reshape(n_rows // PAD, PAD, 512)
        give_back(j)
    ret[PEERS - 1] = ans[PEERS - 1]

    for n in range(4):
        loads[5 + n].wait()
    for j in range(PARTS):
        lo, n_rows = EDGES[j], (EDGES[j + 1] - EDGES[j]) * PAD
        with jax.named_scope(f"rwait{j}"):
            landed(ret, rr_sem, j).wait()
        part = dot(comb[:, pl.ds(lo * PAD, n_rows)], ret[pl.ds(lo, n_rows // PAD)].reshape(n_rows, 1024))
        if j == 0:
            head[...] = part
        elif j < PARTS - 1:
            head[...] += part
        else:
            headb[...] = (head[...] + part).astype(jnp.bfloat16)

    partner = (ys[0] + zh[0] + xs[0], zw[0] + cs[1])
    across = (ys[0] + zh[0] + xs[0], (2 - zw[0]) + cs[0])

    def send(src, dst, ss, rs, b, to):
        return pltpu.make_async_remote_copy(
            src_ref=src.at[b], dst_ref=dst.at[b], send_sem=ss.at[b], recv_sem=rs.at[b],
            device_id=to, device_id_type=MESH,
        )

    def send_z(b):
        return pltpu.make_async_remote_copy(
            src_ref=z_s.at[b], dst_ref=z_r.at[:, pl.ds(b * 256, 256)], send_sem=z_ss.at[b], recv_sem=z_rs.at[b],
            device_id=across, device_id_type=MESH,
        )

    def product(n, b, width=256):
        return dot(headb[...], wm[n, :, pl.ds(b * 256, width)])

    def first(b):
        dd_s[b] = product(0, b).astype(jnp.bfloat16)
        send(dd_s, dd_r, dd_ss, dd_rs, b, partner).start()

    def second(b):
        mine = product(1, b)
        send(dd_s, dd_r, dd_ss, dd_rs, b, partner).wait_recv()
        z_s[b] = (mine + dd_r[b].astype(jnp.float32)).astype(jnp.bfloat16)
        send_z(b).start()

    with jax.named_scope("merge"):
        first(0)
        first(1)
        second(0)
        first(2)
        second(1)
        first(3)
        second(2)
        second(3)
    with jax.named_scope("merge_near"):
        for b in range(4):
            f_s[b] = product(2, b).astype(jnp.bfloat16)
            send(f_s, f_r, f_ss, f_rs, b, partner).start()
        for b in range(2):
            keep[:, pl.ds(b * 512, 512)] = product(3, 2 * b, 512)
        for b in range(4):
            send(f_s, f_r, f_ss, f_rs, b, partner).wait_recv()
            keep[:, pl.ds(b * 256, 256)] += f_r[b].astype(jnp.float32)
        pltpu.make_async_copy(rows(packed, 0, PEERS - 1), rows(packed, 0, PEERS - 1), ds_sem).wait()
        pltpu.make_async_copy(rows(ans, 0, PEERS - 1), rows(ans, 0, PEERS - 1), rs_sem).wait()
        for b in range(4):
            send(dd_s, dd_r, dd_ss, dd_rs, b, partner).wait_send()
            send(f_s, f_r, f_ss, f_rs, b, partner).wait_send()
    with jax.named_scope("final"):
        for b in range(4):
            send_z(b).wait_send()
        for b in range(4):
            send_z(b).wait_recv()


def body(tokens, w_split, w_merge, expert_in, expert_out, expert_ids, combine_q, capacity):
    bf, f32, i32 = jnp.bfloat16, jnp.float32, jnp.int32
    hbm = pl.BlockSpec(memory_space=pl.ANY)
    vm = pl.BlockSpec(memory_space=pltpu.VMEM)
    dma = pltpu.SemaphoreType.DMA
    quarter = pltpu.VMEM((4, 256, 256), bf)
    slots = pltpu.VMEM((PEERS, PAD, 1024), bf)
    mine, other = pl.pallas_call(
        kernel,
        out_shape=[pltpu.VMEM((256, 1024), f32), pltpu.VMEM((256, 1024), bf)],
        in_specs=[hbm] * 9,
        out_specs=[vm, vm],
        scratch_shapes=[
            pltpu.VMEM((2, 256), i32),
            pltpu.VMEM((2, 256), i32),
            pltpu.VMEM((1, 128), i32),
            pltpu.VMEM((1, 128), i32),
            pltpu.VMEM((256, 4096), bf),
            pltpu.VMEM((2, 4096, 512), bf),
            pltpu.VMEM((4, 1024, 1024), bf),
            pltpu.VMEM((1024, 2048), bf),
            pltpu.VMEM((1024, 1024), bf),
            pltpu.VMEM((256, 1024), bf),
            pltpu.VMEM((1024, 256), bf),
            pltpu.VMEM((256, 1024), bf),
            slots,
            slots,
            pltpu.VMEM((max(b - a for a, b in zip(EDGES, EDGES[1:])) * PAD, 1024), bf),
            slots,
            slots,
            pltpu.VMEM((256, 1024), f32),
            pltpu.VMEM((256, 1024), bf),
            quarter, quarter, quarter, quarter, quarter,
            dma((4,)), dma((5,)), dma((4,)), dma, dma((PARTS,)), dma, dma((PARTS,)),
            dma((4,)), dma((4,)), dma((4,)), dma((4,)), dma((4,)), dma((4,)),
        ],
        compiler_params=pltpu.CompilerParams(
            collective_id=0, has_side_effects=True, vmem_limit_bytes=58 * 2**20
        ),
    )(
        expert_ids[0].T,
        combine_q[0].T,
        capacity.reshape(1, -1),
        jnp.asarray(POSITION).reshape(1, -1),
        tokens,
        w_split,
        w_merge,
        expert_in[0],
        expert_out[0],
    )
    return (mine + other.astype(f32)).astype(bf)


def solution(mesh):
    in_specs = (
        P("seq", None),
        P(None, "sub"),
        P("sub", None),
        P(("seq", "sub"), None, None),
        P(("seq", "sub"), None, None),
        P("sub", "seq", None),
        P("sub", "seq", None),
        P(),
    )
    return jax.shard_map(body, mesh=mesh, in_specs=in_specs, out_specs=P("seq", "sub"), check_vma=False)
```

```python
import jax
import jax.numpy as jnp
import numpy as np
from jax import lax
from jax.experimental import pallas as pl
from jax.experimental.pallas import tpu as pltpu
from jax.sharding import PartitionSpec as P

MESH = pl.DeviceIdType.MESH
PEERS = 128
SLOTS = 6
PAD = 8
EDGES = (0, 32, 64, 96, 128)
EARLY = 40
MUL = 45
BLOCKS = ((0, 128), (128, 128), (256, 256), (512, 256), (768, 256))
PARTS = len(EDGES) - 1


def step_of(r):
    return (r // 2) % 4, r // 32, (r // 8) % 4, r % 2


def hops(r):
    return sum((0, 1, 2, 1)[d] for d in step_of(r)[:3])


def mixed():
    return [(i * MUL) % PEERS for i in range(1, PEERS)] + [0]


ORDER = mixed()
POSITION = np.argsort(np.array(ORDER)).astype(np.int32)


def part_of(i):
    return max(j for j in range(PARTS) if EDGES[j] <= i)


def dot(a, b):
    return jnp.dot(a, b, preferred_element_type=jnp.float32)


def kernel(
    ids_h, quota_h, cap_h, table_h, tokens_h, ws_h, wm_h, win_h, wout_h,
    keep, z_r,
    ids, quota, cap, table,
    tokens, ws, wm, win, wout, sub_tok, chosen, comb, packed, recv, act, ans, ret, head, headb,
    dd_s, dd_r, z_s, f_s, f_r,
    sm_sem, ld_sem, wm_sem, ds_sem, dr_sem, rs_sem, rr_sem, dd_ss, dd_rs, z_ss, z_rs, f_ss, f_rs,
):
    s = lax.axis_index("seq")
    u = lax.axis_index("sub")
    mx, my, mz, mc = s % 4, s // 8, ((s // 4) % 2) * 2 + u // 2, u % 2
    zl = mz % 2
    xs = [(mx + d) % 4 for d in range(4)]
    ys = [((my + d) % 4) * 8 for d in range(4)]
    zs = [(mz + d) % 4 for d in range(4)]
    zh = [(z // 2) * 4 for z in zs]
    zw = [(z % 2) * 2 for z in zs]
    cs = [(mc + d) % 2 for d in range(2)]

    def peer(i, sign=1):
        dx, dy, dz, dc = step_of(ORDER[i])
        if sign < 0:
            dx, dy, dz = -dx % 4, -dy % 4, -dz % 4
        return (ys[dy] + zh[dz] + xs[dx], zw[dz] + cs[dc])

    barrier = pltpu.get_barrier_semaphore()

    loads = [pltpu.make_async_copy(tokens_h, tokens, ld_sem.at[0])]
    for n in range(4):
        loads.append(pltpu.make_async_copy(ws_h.at[:, pl.ds(n * 256, 256)], ws.at[n], ld_sem.at[1 + n]))
    small = [
        pltpu.make_async_copy(ids_h, ids, sm_sem.at[0]),
        pltpu.make_async_copy(quota_h, quota, sm_sem.at[1]),
        pltpu.make_async_copy(cap_h, cap, sm_sem.at[2]),
        pltpu.make_async_copy(table_h, table, sm_sem.at[3]),
    ]
    for cp in small:
        cp.start()
    greets = sorted(range(PEERS - 1), key=lambda i: -hops(ORDER[i]))
    for k, i in enumerate(greets):
        if k == 40:
            for cp in loads[:3]:
                cp.start()
        pl.semaphore_signal(barrier, inc=1, device_id=peer(i), device_id_type=MESH)

    loads.append(pltpu.make_async_copy(win_h, win, ld_sem.at[5]))
    loads.append(pltpu.make_async_copy(wout_h, wout, ld_sem.at[6]))
    quarters = [
        (1 - zl) * 2 + (1 - mc),
        (1 - zl) * 2 + mc,
        zl * 2 + (1 - mc),
        zl * 2 + mc,
    ]
    for n in range(4):
        col = pl.multiple_of(quarters[n] * 1024, 1024)
        loads.append(pltpu.make_async_copy(wm_h.at[:, pl.ds(col, 1024)], wm.at[n], wm_sem.at[n]))

    def clear(i, carry):
        ret[pl.ds(i * 8, 8)] = jnp.zeros((8, PAD, 1024), jnp.bfloat16)
        return carry

    lax.fori_loop(0, 16, clear, 0)

    with jax.named_scope("small"):
        for cp in small:
            cp.wait()
    with jax.named_scope("route"):
        e = lax.broadcasted_iota(jnp.int32, (128, 256), 0)
        id0 = ids[0:1, :]
        id1 = ids[1:2, :]
        oh0 = (e == id0).astype(jnp.float32)
        oh1 = (e == id1).astype(jnp.float32)
        tri = (
            lax.broadcasted_iota(jnp.int32, (256, 256), 0) < lax.broadcasted_iota(jnp.int32, (256, 256), 1)
        ).astype(jnp.bfloat16)
        before = dot((oh0 + oh1).astype(jnp.bfloat16), tri)
        rank0 = jnp.sum(oh0 * before, axis=0, keepdims=True)
        rank1 = jnp.sum(oh1 * before, axis=0, keepdims=True)
        sq0 = lax.broadcasted_iota(jnp.int32, (128, 128), 0)
        sq1 = lax.broadcasted_iota(jnp.int32, (128, 128), 1)
        cap_col = jnp.sum(jnp.where(sq0 == sq1, cap[0:1, :].astype(jnp.float32), 0.0), axis=1, keepdims=True)
        ec = sq0 & 1
        ex = (sq0 >> 2) & 3
        ez = ((sq0 >> 4) & 1) * 2 + ((sq0 >> 1) & 1)
        ey = sq0 >> 5
        r = (((ey - my) & 3) << 5) + (((ez - mz) & 3) << 3) + (((ex - mx) & 3) << 1) + ((ec - mc) & 1)
        pos_col = jnp.sum(jnp.where(r == sq1, table[0:1, :].astype(jnp.float32), 0.0), axis=1, keepdims=True)
        lim0 = jnp.sum(oh0 * cap_col, axis=0, keepdims=True)
        lim1 = jnp.sum(oh1 * cap_col, axis=0, keepdims=True)
        loc0 = jnp.sum(oh0 * pos_col, axis=0, keepdims=True) * PAD + rank0
        loc1 = jnp.sum(oh1 * pos_col, axis=0, keepdims=True) * PAD + rank1
        w0 = jnp.where(rank0 < lim0, quota[0:1, :].astype(jnp.float32) * (1.0 / 65536.0), 0.0)
        w1 = jnp.where(rank1 < lim1, quota[1:2, :].astype(jnp.float32) * (1.0 / 65536.0), 0.0)

        for j in range(4):
            p = (lax.broadcasted_iota(jnp.int32, (256, 256), 0) + j * 256).astype(jnp.float32)
            hit = jnp.logical_or(p == loc0, p == loc1)
            chosen[pl.ds(j * 256, 256)] = jnp.where(hit, 1.0, 0.0).astype(jnp.bfloat16)

    def six(ref, i, half):
        return ref.at[i, pl.ds(0, SLOTS), pl.ds(half * 512, 512)]

    def row(ref, i):
        return ref.at[i, pl.ds(0, SLOTS)]

    def rows(ref, i, n):
        return ref.at[pl.ds(i, n), pl.ds(0, SLOTS)]

    def out_to(src, dst, i):
        pltpu.make_async_remote_copy(
            src_ref=src, dst_ref=dst, send_sem=ds_sem, recv_sem=dr_sem.at[part_of(i)],
            device_id=peer(i), device_id_type=MESH,
        ).start()

    loads[0].wait()
    for half in range(2):
        cols = pl.ds(half * 512, 512)
        with jax.named_scope(f"split{half}"):
            for q in (2 * half, 2 * half + 1):
                loads[1 + q].wait()
                if q == 0:
                    loads[3].start()
                    loads[4].start()
                if q == 2:
                    loads[5].start()
                    loads[6].start()
                for m in range(2):
                    top = pl.ds(m * 128, 128)
                    sub_tok[top, pl.ds(q * 256, 256)] = dot(tokens[top, :], ws[q]).astype(jnp.bfloat16)
        with jax.named_scope(f"pack{half}"):
            for j in range(4):
                rows_j = dot(chosen[pl.ds(j * 256, 256)], sub_tok[:, cols]).astype(jnp.bfloat16)
                packed[pl.ds(j * 32, 32), :, cols] = rows_j.reshape(32, PAD, 512)
        with jax.named_scope(f"send{half}"):
            if half == 0:
                pl.semaphore_wait(barrier, PEERS - 1)
            for i in range(EARLY):
                out_to(six(packed, i, half), six(recv, i, half), i)
    with jax.named_scope("send_rest"):
        for i in range(EARLY, PEERS - 1):
            out_to(row(packed, i), row(recv, i), i)
    for cp in loads[7:]:
        cp.start()
    recv[PEERS - 1] = packed[PEERS - 1]

    with jax.named_scope("comb"):
        stacked = jnp.concatenate([loc0, loc1, w0, w1, jnp.zeros((4, 256), jnp.float32)], axis=0)
        turned = stacked.T
        l0 = turned[:, 0:1]
        l1 = turned[:, 1:2]
        v0 = turned[:, 2:3]
        v1 = turned[:, 3:4]
        for j in range(4):
            p = (lax.broadcasted_iota(jnp.int32, (256, 256), 1) + j * 256).astype(jnp.float32)
            c = jnp.where(p == l0, v0, jnp.where(p == l1, v1, 0.0))
            comb[:, pl.ds(j * 256, 256)] = c.astype(jnp.bfloat16)

    loads[5].wait()
    loads[6].wait()

    def landed(ref, sem, j):
        lo, hi = EDGES[j], min(EDGES[j + 1], PEERS - 1)
        return pltpu.make_async_copy(rows(ref, lo, hi - lo), rows(ref, lo, hi - lo), sem.at[j])

    def give_back(j):
        with jax.named_scope(f"back{j}"):
            for i in range(EDGES[j], min(EDGES[j + 1], PEERS - 1)):
                pltpu.make_async_remote_copy(
                    src_ref=row(ans, i), dst_ref=row(ret, i),
                    send_sem=rs_sem, recv_sem=rr_sem.at[j],
                    device_id=peer(i, -1), device_id_type=MESH,
                ).start()

    for j in range(PARTS):
        lo, n_rows = EDGES[j], (EDGES[j + 1] - EDGES[j]) * PAD
        with jax.named_scope(f"wait{j}"):
            landed(recv, dr_sem, j).wait()
        with jax.named_scope(f"ffn{j}"):
            x = recv[pl.ds(lo, n_rows // PAD)].reshape(n_rows, 1024)
            for n in range(4):
                g = dot(x, win[:, pl.ds(n * 256, 256)])
                t = dot(x, win[:, pl.ds(1024 + n * 256, 256)])
                act[pl.ds(0, n_rows), pl.ds(n * 256, 256)] = (g / (1.0 + jnp.exp(-g)) * t).astype(jnp.bfloat16)
            for n in range(2):
                a = dot(act[pl.ds(0, n_rows)], wout[:, pl.ds(n * 512, 512)]).astype(jnp.bfloat16)
                ans[pl.ds(lo, n_rows // PAD), :, pl.ds(n * 512, 512)] = a.reshape(n_rows // PAD, PAD, 512)
        give_back(j)
    ret[PEERS - 1] = ans[PEERS - 1]

    for n in range(4):
        loads[7 + n].wait()
    for j in range(PARTS):
        lo, n_rows = EDGES[j], (EDGES[j + 1] - EDGES[j]) * PAD
        with jax.named_scope(f"rwait{j}"):
            landed(ret, rr_sem, j).wait()
        part = dot(comb[:, pl.ds(lo * PAD, n_rows)], ret[pl.ds(lo, n_rows // PAD)].reshape(n_rows, 1024))
        if j == 0:
            head[...] = part
        elif j < PARTS - 1:
            head[...] += part
        else:
            headb[...] = (head[...] + part).astype(jnp.bfloat16)

    partner = (ys[0] + zh[0] + xs[0], zw[0] + cs[1])
    across = (ys[0] + zh[0] + xs[0], (2 - zw[0]) + cs[0])

    def send(src, dst, ss, rs, b, to):
        cols = pl.ds(*BLOCKS[b])
        return pltpu.make_async_remote_copy(
            src_ref=src.at[:, cols], dst_ref=dst.at[:, cols], send_sem=ss.at[b], recv_sem=rs.at[b],
            device_id=to, device_id_type=MESH,
        )

    def send_dd(b):
        return send(dd_s, dd_r, dd_ss, dd_rs, b, partner)

    def send_f(b):
        return send(f_s, f_r, f_ss, f_rs, b, partner)

    def send_z(b):
        return send(z_s, z_r, z_ss, z_rs, b, across)

    tops = (pl.ds(0, 128), pl.ds(128, 128))

    def product(n, b, top):
        return dot(headb[top, :], wm[n, :, pl.ds(*BLOCKS[b])])

    def first(b):
        for top in tops:
            dd_s[top, pl.ds(*BLOCKS[b])] = product(0, b, top).astype(jnp.bfloat16)
        send_dd(b).start()

    def own(b):
        for top in tops:
            head[top, pl.ds(*BLOCKS[b])] = product(1, b, top)

    def second(b):
        cols = pl.ds(*BLOCKS[b])
        send_dd(b).wait_recv()
        z_s[:, cols] = (head[:, cols] + dd_r[:, cols].astype(jnp.float32)).astype(jnp.bfloat16)
        send_z(b).start()

    blocks = range(len(BLOCKS))
    with jax.named_scope("merge"):
        first(0)
        own(0)
        first(1)
        own(1)
        second(0)
        first(2)
        second(1)
        own(2)
        first(3)
        second(2)
        own(3)
        first(4)
        second(3)
        own(4)
        second(4)
    with jax.named_scope("merge_near"):
        for b in blocks:
            for top in tops:
                f_s[top, pl.ds(*BLOCKS[b])] = product(2, b, top).astype(jnp.bfloat16)
            send_f(b).start()
        for b in range(2):
            keep[:, pl.ds(b * 512, 512)] = dot(headb[...], wm[3, :, pl.ds(b * 512, 512)])
        for b in blocks:
            cols = pl.ds(*BLOCKS[b])
            send_f(b).wait_recv()
            keep[:, cols] += f_r[:, cols].astype(jnp.float32)
        pltpu.make_async_copy(rows(packed, 0, PEERS - 1), rows(packed, 0, PEERS - 1), ds_sem).wait()
        pltpu.make_async_copy(rows(ans, 0, PEERS - 1), rows(ans, 0, PEERS - 1), rs_sem).wait()
        for b in blocks:
            send_dd(b).wait_send()
            send_f(b).wait_send()
    with jax.named_scope("final"):
        for b in blocks:
            send_z(b).wait_send()
        for b in blocks:
            send_z(b).wait_recv()


def body(tokens, w_split, w_merge, expert_in, expert_out, expert_ids, combine_q, capacity):
    bf, f32, i32 = jnp.bfloat16, jnp.float32, jnp.int32
    hbm = pl.BlockSpec(memory_space=pl.ANY)
    vm = pl.BlockSpec(memory_space=pltpu.VMEM)
    dma = pltpu.SemaphoreType.DMA
    quarter = pltpu.VMEM((256, 1024), bf)
    per_block = dma((len(BLOCKS),))
    slots = pltpu.VMEM((PEERS, PAD, 1024), bf)
    mine, other = pl.pallas_call(
        kernel,
        out_shape=[pltpu.VMEM((256, 1024), f32), pltpu.VMEM((256, 1024), bf)],
        in_specs=[hbm] * 9,
        out_specs=[vm, vm],
        scratch_shapes=[
            pltpu.VMEM((2, 256), i32),
            pltpu.VMEM((2, 256), i32),
            pltpu.VMEM((1, 128), i32),
            pltpu.VMEM((1, 128), i32),
            pltpu.VMEM((256, 4096), bf),
            pltpu.VMEM((4, 4096, 256), bf),
            pltpu.VMEM((4, 1024, 1024), bf),
            pltpu.VMEM((1024, 2048), bf),
            pltpu.VMEM((1024, 1024), bf),
            pltpu.VMEM((256, 1024), bf),
            pltpu.VMEM((1024, 256), bf),
            pltpu.VMEM((256, 1024), bf),
            slots,
            slots,
            pltpu.VMEM((max(b - a for a, b in zip(EDGES, EDGES[1:])) * PAD, 1024), bf),
            slots,
            slots,
            pltpu.VMEM((256, 1024), f32),
            pltpu.VMEM((256, 1024), bf),
            quarter, quarter, quarter, quarter, quarter,
            dma((4,)), dma((7,)), dma((4,)), dma, dma((PARTS,)), dma, dma((PARTS,)),
            per_block, per_block, per_block, per_block, per_block, per_block,
        ],
        compiler_params=pltpu.CompilerParams(
            collective_id=0, has_side_effects=True, vmem_limit_bytes=58 * 2**20
        ),
    )(
        expert_ids[0].T,
        combine_q[0].T,
        capacity.reshape(1, -1),
        jnp.asarray(POSITION).reshape(1, -1),
        tokens,
        w_split,
        w_merge,
        expert_in[0],
        expert_out[0],
    )
    return (mine + other.astype(f32)).astype(bf)


def solution(mesh):
    in_specs = (
        P("seq", None),
        P(None, "sub"),
        P("sub", None),
        P(("seq", "sub"), None, None),
        P(("seq", "sub"), None, None),
        P("sub", "seq", None),
        P("sub", "seq", None),
        P(),
    )
    return jax.shard_map(body, mesh=mesh, in_specs=in_specs, out_specs=P("seq", "sub"), check_vma=False)
```

```python
import jax
import jax.numpy as jnp
import numpy as np
from jax import lax
from jax.experimental import pallas as pl
from jax.experimental.pallas import tpu as pltpu
from jax.sharding import PartitionSpec as P

MESH = pl.DeviceIdType.MESH
PEERS = 128
SLOTS = 6
PAD = 8
EDGES = (0, 32, 64, 96, 128)
EARLY = 40
MUL = 45
BLOCKS = ((0, 128), (128, 128), (256, 256), (512, 256), (768, 256))
PARTS = len(EDGES) - 1


def step_of(r):
    return (r // 2) % 4, r // 32, (r // 8) % 4, r % 2


def hops(r):
    return sum((0, 1, 2, 1)[d] for d in step_of(r)[:3])


def mixed():
    steps = [(i * MUL) % PEERS for i in range(1, PEERS)]
    runs = [steps[k : k + 32] for k in range(0, PEERS - 1, 32)]
    return [r for run in runs for r in sorted(run, key=lambda r: -hops(r))] + [0]


ORDER = mixed()
POSITION = np.argsort(np.array(ORDER)).astype(np.int32)


def part_of(i):
    return max(j for j in range(PARTS) if EDGES[j] <= i)


def dot(a, b):
    return jnp.dot(a, b, preferred_element_type=jnp.float32)


def kernel(
    ids_h, quota_h, cap_h, table_h, tokens_h, ws_h, wm_h, win_h, wout_h,
    keep, z_r,
    ids, quota, cap, table,
    tokens, ws, wm, win, wout, sub_tok, chosen, comb, packed, recv, act, ans, ret, head, headb,
    dd_s, dd_r, z_s, f_s, f_r,
    sm_sem, ld_sem, wm_sem, ds_sem, dr_sem, rs_sem, rr_sem, dd_ss, dd_rs, z_ss, z_rs, f_ss, f_rs,
):
    s = lax.axis_index("seq")
    u = lax.axis_index("sub")
    mx, my, mz, mc = s % 4, s // 8, ((s // 4) % 2) * 2 + u // 2, u % 2
    zl = mz % 2
    xs = [(mx + d) % 4 for d in range(4)]
    ys = [((my + d) % 4) * 8 for d in range(4)]
    zs = [(mz + d) % 4 for d in range(4)]
    zh = [(z // 2) * 4 for z in zs]
    zw = [(z % 2) * 2 for z in zs]
    cs = [(mc + d) % 2 for d in range(2)]

    def peer(i, sign=1):
        dx, dy, dz, dc = step_of(ORDER[i])
        if sign < 0:
            dx, dy, dz = -dx % 4, -dy % 4, -dz % 4
        return (ys[dy] + zh[dz] + xs[dx], zw[dz] + cs[dc])

    barrier = pltpu.get_barrier_semaphore()

    loads = [pltpu.make_async_copy(tokens_h, tokens, ld_sem.at[0])]
    for n in range(4):
        loads.append(pltpu.make_async_copy(ws_h.at[:, pl.ds(n * 256, 256)], ws.at[n], ld_sem.at[1 + n]))
    small = [
        pltpu.make_async_copy(ids_h, ids, sm_sem.at[0]),
        pltpu.make_async_copy(quota_h, quota, sm_sem.at[1]),
        pltpu.make_async_copy(cap_h, cap, sm_sem.at[2]),
        pltpu.make_async_copy(table_h, table, sm_sem.at[3]),
    ]
    for cp in small:
        cp.start()
    greets = sorted(range(PEERS - 1), key=lambda i: -hops(ORDER[i]))
    for k, i in enumerate(greets):
        if k == 40:
            for cp in loads[:3]:
                cp.start()
        pl.semaphore_signal(barrier, inc=1, device_id=peer(i), device_id_type=MESH)

    loads.append(pltpu.make_async_copy(win_h, win, ld_sem.at[5]))
    loads.append(pltpu.make_async_copy(wout_h, wout, ld_sem.at[6]))
    quarters = [
        (1 - zl) * 2 + (1 - mc),
        (1 - zl) * 2 + mc,
        zl * 2 + (1 - mc),
        zl * 2 + mc,
    ]
    for n in range(4):
        col = pl.multiple_of(quarters[n] * 1024, 1024)
        loads.append(pltpu.make_async_copy(wm_h.at[:, pl.ds(col, 1024)], wm.at[n], wm_sem.at[n]))

    def clear(i, carry):
        ret[pl.ds(i * 8, 8)] = jnp.zeros((8, PAD, 1024), jnp.bfloat16)
        return carry

    lax.fori_loop(0, 16, clear, 0)

    with jax.named_scope("small"):
        for cp in small:
            cp.wait()
    with jax.named_scope("route"):
        e = lax.broadcasted_iota(jnp.int32, (128, 256), 0)
        id0 = ids[0:1, :]
        id1 = ids[1:2, :]
        oh0 = (e == id0).astype(jnp.float32)
        oh1 = (e == id1).astype(jnp.float32)
        tri = (
            lax.broadcasted_iota(jnp.int32, (256, 256), 0) < lax.broadcasted_iota(jnp.int32, (256, 256), 1)
        ).astype(jnp.bfloat16)
        before = dot((oh0 + oh1).astype(jnp.bfloat16), tri)
        rank0 = jnp.sum(oh0 * before, axis=0, keepdims=True)
        rank1 = jnp.sum(oh1 * before, axis=0, keepdims=True)
        sq0 = lax.broadcasted_iota(jnp.int32, (128, 128), 0)
        sq1 = lax.broadcasted_iota(jnp.int32, (128, 128), 1)
        cap_col = jnp.sum(jnp.where(sq0 == sq1, cap[0:1, :].astype(jnp.float32), 0.0), axis=1, keepdims=True)
        ec = sq0 & 1
        ex = (sq0 >> 2) & 3
        ez = ((sq0 >> 4) & 1) * 2 + ((sq0 >> 1) & 1)
        ey = sq0 >> 5
        r = (((ey - my) & 3) << 5) + (((ez - mz) & 3) << 3) + (((ex - mx) & 3) << 1) + ((ec - mc) & 1)
        pos_col = jnp.sum(jnp.where(r == sq1, table[0:1, :].astype(jnp.float32), 0.0), axis=1, keepdims=True)
        lim0 = jnp.sum(oh0 * cap_col, axis=0, keepdims=True)
        lim1 = jnp.sum(oh1 * cap_col, axis=0, keepdims=True)
        loc0 = jnp.sum(oh0 * pos_col, axis=0, keepdims=True) * PAD + rank0
        loc1 = jnp.sum(oh1 * pos_col, axis=0, keepdims=True) * PAD + rank1
        w0 = jnp.where(rank0 < lim0, quota[0:1, :].astype(jnp.float32) * (1.0 / 65536.0), 0.0)
        w1 = jnp.where(rank1 < lim1, quota[1:2, :].astype(jnp.float32) * (1.0 / 65536.0), 0.0)

        for j in range(4):
            p = (lax.broadcasted_iota(jnp.int32, (256, 256), 0) + j * 256).astype(jnp.float32)
            hit = jnp.logical_or(p == loc0, p == loc1)
            chosen[pl.ds(j * 256, 256)] = jnp.where(hit, 1.0, 0.0).astype(jnp.bfloat16)

    def six(ref, i, half):
        return ref.at[i, pl.ds(0, SLOTS), pl.ds(half * 512, 512)]

    def row(ref, i):
        return ref.at[i, pl.ds(0, SLOTS)]

    def rows(ref, i, n):
        return ref.at[pl.ds(i, n), pl.ds(0, SLOTS)]

    def out_to(src, dst, i):
        pltpu.make_async_remote_copy(
            src_ref=src, dst_ref=dst, send_sem=ds_sem, recv_sem=dr_sem.at[part_of(i)],
            device_id=peer(i), device_id_type=MESH,
        ).start()

    loads[0].wait()
    for half in range(2):
        cols = pl.ds(half * 512, 512)
        with jax.named_scope(f"split{half}"):
            for q in (2 * half, 2 * half + 1):
                loads[1 + q].wait()
                if q == 0:
                    loads[3].start()
                    loads[4].start()
                if q == 2:
                    loads[5].start()
                    loads[6].start()
                for m in range(2):
                    top = pl.ds(m * 128, 128)
                    sub_tok[top, pl.ds(q * 256, 256)] = dot(tokens[top, :], ws[q]).astype(jnp.bfloat16)
        with jax.named_scope(f"pack{half}"):
            for j in range(4):
                rows_j = dot(chosen[pl.ds(j * 256, 256)], sub_tok[:, cols]).astype(jnp.bfloat16)
                packed[pl.ds(j * 32, 32), :, cols] = rows_j.reshape(32, PAD, 512)
        with jax.named_scope(f"send{half}"):
            if half == 0:
                pl.semaphore_wait(barrier, PEERS - 1)
            for i in range(EARLY):
                out_to(six(packed, i, half), six(recv, i, half), i)
    with jax.named_scope("send_rest"):
        for i in range(EARLY, PEERS - 1):
            out_to(row(packed, i), row(recv, i), i)
    for cp in loads[7:]:
        cp.start()
    recv[PEERS - 1] = packed[PEERS - 1]

    with jax.named_scope("comb"):
        stacked = jnp.concatenate([loc0, loc1, w0, w1, jnp.zeros((4, 256), jnp.float32)], axis=0)
        turned = stacked.T
        l0 = turned[:, 0:1]
        l1 = turned[:, 1:2]
        v0 = turned[:, 2:3]
        v1 = turned[:, 3:4]
        for j in range(4):
            p = (lax.broadcasted_iota(jnp.int32, (256, 256), 1) + j * 256).astype(jnp.float32)
            c = jnp.where(p == l0, v0, jnp.where(p == l1, v1, 0.0))
            comb[:, pl.ds(j * 256, 256)] = c.astype(jnp.bfloat16)

    loads[5].wait()
    loads[6].wait()

    def landed(ref, sem, j):
        lo, hi = EDGES[j], min(EDGES[j + 1], PEERS - 1)
        return pltpu.make_async_copy(rows(ref, lo, hi - lo), rows(ref, lo, hi - lo), sem.at[j])

    def give_back(j):
        with jax.named_scope(f"back{j}"):
            for i in range(EDGES[j], min(EDGES[j + 1], PEERS - 1)):
                pltpu.make_async_remote_copy(
                    src_ref=row(ans, i), dst_ref=row(ret, i),
                    send_sem=rs_sem, recv_sem=rr_sem.at[j],
                    device_id=peer(i, -1), device_id_type=MESH,
                ).start()

    for j in range(PARTS):
        lo, n_rows = EDGES[j], (EDGES[j + 1] - EDGES[j]) * PAD
        with jax.named_scope(f"wait{j}"):
            landed(recv, dr_sem, j).wait()
        with jax.named_scope(f"ffn{j}"):
            x = recv[pl.ds(lo, n_rows // PAD)].reshape(n_rows, 1024)
            for n in range(4):
                g = dot(x, win[:, pl.ds(n * 256, 256)])
                t = dot(x, win[:, pl.ds(1024 + n * 256, 256)])
                act[pl.ds(0, n_rows), pl.ds(n * 256, 256)] = (g / (1.0 + jnp.exp(-g)) * t).astype(jnp.bfloat16)
            for n in range(2):
                a = dot(act[pl.ds(0, n_rows)], wout[:, pl.ds(n * 512, 512)]).astype(jnp.bfloat16)
                ans[pl.ds(lo, n_rows // PAD), :, pl.ds(n * 512, 512)] = a.reshape(n_rows // PAD, PAD, 512)
        give_back(j)
    ret[PEERS - 1] = ans[PEERS - 1]

    for n in range(4):
        loads[7 + n].wait()
    for j in range(PARTS):
        lo, n_rows = EDGES[j], (EDGES[j + 1] - EDGES[j]) * PAD
        with jax.named_scope(f"rwait{j}"):
            landed(ret, rr_sem, j).wait()
        part = dot(comb[:, pl.ds(lo * PAD, n_rows)], ret[pl.ds(lo, n_rows // PAD)].reshape(n_rows, 1024))
        if j == 0:
            head[...] = part
        elif j < PARTS - 1:
            head[...] += part
        else:
            headb[...] = (head[...] + part).astype(jnp.bfloat16)

    partner = (ys[0] + zh[0] + xs[0], zw[0] + cs[1])
    across = (ys[0] + zh[0] + xs[0], (2 - zw[0]) + cs[0])

    def send(src, dst, ss, rs, b, to):
        cols = pl.ds(*BLOCKS[b])
        return pltpu.make_async_remote_copy(
            src_ref=src.at[:, cols], dst_ref=dst.at[:, cols], send_sem=ss.at[b], recv_sem=rs.at[b],
            device_id=to, device_id_type=MESH,
        )

    def send_dd(b):
        return send(dd_s, dd_r, dd_ss, dd_rs, b, partner)

    def send_f(b):
        return send(f_s, f_r, f_ss, f_rs, b, partner)

    def send_z(b):
        return send(z_s, z_r, z_ss, z_rs, b, across)

    tops = (pl.ds(0, 128), pl.ds(128, 128))

    def product(n, b, top):
        return dot(headb[top, :], wm[n, :, pl.ds(*BLOCKS[b])])

    def first(b):
        for top in tops:
            dd_s[top, pl.ds(*BLOCKS[b])] = product(0, b, top).astype(jnp.bfloat16)
        send_dd(b).start()

    def own(b):
        for top in tops:
            head[top, pl.ds(*BLOCKS[b])] = product(1, b, top)

    def second(b):
        cols = pl.ds(*BLOCKS[b])
        send_dd(b).wait_recv()
        z_s[:, cols] = (head[:, cols] + dd_r[:, cols].astype(jnp.float32)).astype(jnp.bfloat16)
        send_z(b).start()

    blocks = range(len(BLOCKS))
    with jax.named_scope("merge"):
        first(0)
        own(0)
        first(1)
        own(1)
        second(0)
        first(2)
        second(1)
        own(2)
        first(3)
        second(2)
        own(3)
        first(4)
        second(3)
        own(4)
        second(4)
    with jax.named_scope("merge_near"):
        for b in blocks:
            for top in tops:
                f_s[top, pl.ds(*BLOCKS[b])] = product(2, b, top).astype(jnp.bfloat16)
            send_f(b).start()
        for b in range(2):
            keep[:, pl.ds(b * 512, 512)] = dot(headb[...], wm[3, :, pl.ds(b * 512, 512)])
        for b in blocks:
            cols = pl.ds(*BLOCKS[b])
            send_f(b).wait_recv()
            keep[:, cols] += f_r[:, cols].astype(jnp.float32)
        pltpu.make_async_copy(rows(packed, 0, PEERS - 1), rows(packed, 0, PEERS - 1), ds_sem).wait()
        pltpu.make_async_copy(rows(ans, 0, PEERS - 1), rows(ans, 0, PEERS - 1), rs_sem).wait()
        for b in blocks:
            send_dd(b).wait_send()
            send_f(b).wait_send()
    with jax.named_scope("final"):
        for b in blocks:
            send_z(b).wait_send()
        for b in blocks:
            send_z(b).wait_recv()


def body(tokens, w_split, w_merge, expert_in, expert_out, expert_ids, combine_q, capacity):
    bf, f32, i32 = jnp.bfloat16, jnp.float32, jnp.int32
    hbm = pl.BlockSpec(memory_space=pl.ANY)
    vm = pl.BlockSpec(memory_space=pltpu.VMEM)
    dma = pltpu.SemaphoreType.DMA
    quarter = pltpu.VMEM((256, 1024), bf)
    per_block = dma((len(BLOCKS),))
    slots = pltpu.VMEM((PEERS, PAD, 1024), bf)
    mine, other = pl.pallas_call(
        kernel,
        out_shape=[pltpu.VMEM((256, 1024), f32), pltpu.VMEM((256, 1024), bf)],
        in_specs=[hbm] * 9,
        out_specs=[vm, vm],
        scratch_shapes=[
            pltpu.VMEM((2, 256), i32),
            pltpu.VMEM((2, 256), i32),
            pltpu.VMEM((1, 128), i32),
            pltpu.VMEM((1, 128), i32),
            pltpu.VMEM((256, 4096), bf),
            pltpu.VMEM((4, 4096, 256), bf),
            pltpu.VMEM((4, 1024, 1024), bf),
            pltpu.VMEM((1024, 2048), bf),
            pltpu.VMEM((1024, 1024), bf),
            pltpu.VMEM((256, 1024), bf),
            pltpu.VMEM((1024, 256), bf),
            pltpu.VMEM((256, 1024), bf),
            slots,
            slots,
            pltpu.VMEM((max(b - a for a, b in zip(EDGES, EDGES[1:])) * PAD, 1024), bf),
            slots,
            slots,
            pltpu.VMEM((256, 1024), f32),
            pltpu.VMEM((256, 1024), bf),
            quarter, quarter, quarter, quarter, quarter,
            dma((4,)), dma((7,)), dma((4,)), dma, dma((PARTS,)), dma, dma((PARTS,)),
            per_block, per_block, per_block, per_block, per_block, per_block,
        ],
        compiler_params=pltpu.CompilerParams(
            collective_id=0, has_side_effects=True, vmem_limit_bytes=58 * 2**20
        ),
    )(
        expert_ids[0].T,
        combine_q[0].T,
        capacity.reshape(1, -1),
        jnp.asarray(POSITION).reshape(1, -1),
        tokens,
        w_split,
        w_merge,
        expert_in[0],
        expert_out[0],
    )
    return (mine + other.astype(f32)).astype(bf)


def solution(mesh):
    in_specs = (
        P("seq", None),
        P(None, "sub"),
        P("sub", None),
        P(("seq", "sub"), None, None),
        P(("seq", "sub"), None, None),
        P("sub", "seq", None),
        P("sub", "seq", None),
        P(),
    )
    return jax.shard_map(body, mesh=mesh, in_specs=in_specs, out_specs=P("seq", "sub"), check_vma=False)
```

```python
import jax
import jax.numpy as jnp
import numpy as np
from jax import lax
from jax.experimental import pallas as pl
from jax.experimental.pallas import tpu as pltpu
from jax.sharding import PartitionSpec as P

MESH = pl.DeviceIdType.MESH
PEERS = 128
SLOTS = 6
PAD = 8
EDGES = (0, 32, 64, 96, 128)
EARLY = 32
MUL = 45
BLOCKS = ((0, 128), (128, 128), (256, 256), (512, 256), (768, 256))
PARTS = len(EDGES) - 1


def step_of(r):
    return (r // 2) % 4, r // 32, (r // 8) % 4, r % 2


def hops(r):
    return sum((0, 1, 2, 1)[d] for d in step_of(r)[:3])


def mixed():
    steps = [(i * MUL) % PEERS for i in range(1, PEERS)]
    runs = [steps[k : k + 32] for k in range(0, PEERS - 1, 32)]
    return [r for run in runs for r in sorted(run, key=lambda r: -hops(r))] + [0]


ORDER = mixed()
POSITION = np.argsort(np.array(ORDER)).astype(np.int32)


def part_of(i):
    return max(j for j in range(PARTS) if EDGES[j] <= i)


def dot(a, b):
    return jnp.dot(a, b, preferred_element_type=jnp.float32)


def kernel(
    ids_h, quota_h, cap_h, table_h, tokens_h, ws_h, wm_h, win_h, wout_h,
    keep, z_r,
    ids, quota, cap, table,
    tokens, ws, wm, win, wout, sub_tok, chosen, comb, packed, recv, act, ans, ret, head, headb,
    dd_s, dd_r, z_s, f_s, f_r,
    sm_sem, ld_sem, wm_sem, ds_sem, dr_sem, rs_sem, rr_sem, dd_ss, dd_rs, z_ss, z_rs, f_ss, f_rs,
):
    s = lax.axis_index("seq")
    u = lax.axis_index("sub")
    mx, my, mz, mc = s % 4, s // 8, ((s // 4) % 2) * 2 + u // 2, u % 2
    zl = mz % 2
    xs = [(mx + d) % 4 for d in range(4)]
    ys = [((my + d) % 4) * 8 for d in range(4)]
    zs = [(mz + d) % 4 for d in range(4)]
    zh = [(z // 2) * 4 for z in zs]
    zw = [(z % 2) * 2 for z in zs]
    cs = [(mc + d) % 2 for d in range(2)]

    def peer(i, sign=1):
        dx, dy, dz, dc = step_of(ORDER[i])
        if sign < 0:
            dx, dy, dz = -dx % 4, -dy % 4, -dz % 4
        return (ys[dy] + zh[dz] + xs[dx], zw[dz] + cs[dc])

    barrier = pltpu.get_barrier_semaphore()

    loads = [pltpu.make_async_copy(tokens_h, tokens, ld_sem.at[0])]
    for n in range(4):
        loads.append(pltpu.make_async_copy(ws_h.at[:, pl.ds(n * 256, 256)], ws.at[n], ld_sem.at[1 + n]))
    small = [
        pltpu.make_async_copy(ids_h, ids, sm_sem.at[0]),
        pltpu.make_async_copy(quota_h, quota, sm_sem.at[1]),
        pltpu.make_async_copy(cap_h, cap, sm_sem.at[2]),
        pltpu.make_async_copy(table_h, table, sm_sem.at[3]),
    ]
    for cp in small:
        cp.start()
    greets = sorted(range(PEERS - 1), key=lambda i: -hops(ORDER[i]))
    for k, i in enumerate(greets):
        if k == 40:
            for cp in loads[:3]:
                cp.start()
        pl.semaphore_signal(barrier, inc=1, device_id=peer(i), device_id_type=MESH)

    loads.append(pltpu.make_async_copy(win_h, win, ld_sem.at[5]))
    loads.append(pltpu.make_async_copy(wout_h, wout, ld_sem.at[6]))
    quarters = [
        (1 - zl) * 2 + (1 - mc),
        (1 - zl) * 2 + mc,
        zl * 2 + (1 - mc),
        zl * 2 + mc,
    ]
    for n in range(4):
        col = pl.multiple_of(quarters[n] * 1024, 1024)
        loads.append(pltpu.make_async_copy(wm_h.at[:, pl.ds(col, 1024)], wm.at[n], wm_sem.at[n]))

    def clear(i, carry):
        ret[pl.ds(i * 8, 8)] = jnp.zeros((8, PAD, 1024), jnp.bfloat16)
        return carry

    lax.fori_loop(0, 16, clear, 0)

    with jax.named_scope("small"):
        for cp in small:
            cp.wait()
    with jax.named_scope("route"):
        e = lax.broadcasted_iota(jnp.int32, (128, 256), 0)
        id0 = ids[0:1, :]
        id1 = ids[1:2, :]
        oh0 = (e == id0).astype(jnp.float32)
        oh1 = (e == id1).astype(jnp.float32)
        tri = (
            lax.broadcasted_iota(jnp.int32, (256, 256), 0) < lax.broadcasted_iota(jnp.int32, (256, 256), 1)
        ).astype(jnp.bfloat16)
        before = dot((oh0 + oh1).astype(jnp.bfloat16), tri)
        rank0 = jnp.sum(oh0 * before, axis=0, keepdims=True)
        rank1 = jnp.sum(oh1 * before, axis=0, keepdims=True)
        sq0 = lax.broadcasted_iota(jnp.int32, (128, 128), 0)
        sq1 = lax.broadcasted_iota(jnp.int32, (128, 128), 1)
        cap_col = jnp.sum(jnp.where(sq0 == sq1, cap[0:1, :].astype(jnp.float32), 0.0), axis=1, keepdims=True)
        ec = sq0 & 1
        ex = (sq0 >> 2) & 3
        ez = ((sq0 >> 4) & 1) * 2 + ((sq0 >> 1) & 1)
        ey = sq0 >> 5
        r = (((ey - my) & 3) << 5) + (((ez - mz) & 3) << 3) + (((ex - mx) & 3) << 1) + ((ec - mc) & 1)
        pos_col = jnp.sum(jnp.where(r == sq1, table[0:1, :].astype(jnp.float32), 0.0), axis=1, keepdims=True)
        lim0 = jnp.sum(oh0 * cap_col, axis=0, keepdims=True)
        lim1 = jnp.sum(oh1 * cap_col, axis=0, keepdims=True)
        loc0 = jnp.sum(oh0 * pos_col, axis=0, keepdims=True) * PAD + rank0
        loc1 = jnp.sum(oh1 * pos_col, axis=0, keepdims=True) * PAD + rank1
        w0 = jnp.where(rank0 < lim0, quota[0:1, :].astype(jnp.float32) * (1.0 / 65536.0), 0.0)
        w1 = jnp.where(rank1 < lim1, quota[1:2, :].astype(jnp.float32) * (1.0 / 65536.0), 0.0)

        for j in range(4):
            p = (lax.broadcasted_iota(jnp.int32, (256, 256), 0) + j * 256).astype(jnp.float32)
            hit = jnp.logical_or(p == loc0, p == loc1)
            chosen[pl.ds(j * 256, 256)] = jnp.where(hit, 1.0, 0.0).astype(jnp.bfloat16)

    def six(ref, i, half):
        return ref.at[i, pl.ds(0, SLOTS), pl.ds(half * 512, 512)]

    def row(ref, i):
        return ref.at[i, pl.ds(0, SLOTS)]

    def rows(ref, i, n):
        return ref.at[pl.ds(i, n), pl.ds(0, SLOTS)]

    def out_to(src, dst, i):
        pltpu.make_async_remote_copy(
            src_ref=src, dst_ref=dst, send_sem=ds_sem, recv_sem=dr_sem.at[part_of(i)],
            device_id=peer(i), device_id_type=MESH,
        ).start()

    loads[0].wait()
    for half in range(2):
        cols = pl.ds(half * 512, 512)
        with jax.named_scope(f"split{half}"):
            for q in (2 * half, 2 * half + 1):
                loads[1 + q].wait()
                if q == 0:
                    loads[3].start()
                    loads[4].start()
                if q == 2:
                    loads[5].start()
                    loads[6].start()
                for m in range(2):
                    top = pl.ds(m * 128, 128)
                    sub_tok[top, pl.ds(q * 256, 256)] = dot(tokens[top, :], ws[q]).astype(jnp.bfloat16)
        with jax.named_scope(f"pack{half}"):
            for j in range(4):
                rows_j = dot(chosen[pl.ds(j * 256, 256)], sub_tok[:, cols]).astype(jnp.bfloat16)
                packed[pl.ds(j * 32, 32), :, cols] = rows_j.reshape(32, PAD, 512)
        with jax.named_scope(f"send{half}"):
            if half == 0:
                pl.semaphore_wait(barrier, PEERS - 1)
            for i in range(EARLY):
                out_to(six(packed, i, half), six(recv, i, half), i)
    with jax.named_scope("send_rest"):
        for i in range(EARLY, PEERS - 1):
            out_to(row(packed, i), row(recv, i), i)
    for cp in loads[7:]:
        cp.start()
    recv[PEERS - 1] = packed[PEERS - 1]

    with jax.named_scope("comb"):
        stacked = jnp.concatenate([loc0, loc1, w0, w1, jnp.zeros((4, 256), jnp.float32)], axis=0)
        turned = stacked.T
        l0 = turned[:, 0:1]
        l1 = turned[:, 1:2]
        v0 = turned[:, 2:3]
        v1 = turned[:, 3:4]
        for j in range(4):
            p = (lax.broadcasted_iota(jnp.int32, (256, 256), 1) + j * 256).astype(jnp.float32)
            c = jnp.where(p == l0, v0, jnp.where(p == l1, v1, 0.0))
            comb[:, pl.ds(j * 256, 256)] = c.astype(jnp.bfloat16)

    loads[5].wait()
    loads[6].wait()

    def landed(ref, sem, j):
        lo, hi = EDGES[j], min(EDGES[j + 1], PEERS - 1)
        return pltpu.make_async_copy(rows(ref, lo, hi - lo), rows(ref, lo, hi - lo), sem.at[j])

    def give_back(j):
        with jax.named_scope(f"back{j}"):
            for i in range(EDGES[j], min(EDGES[j + 1], PEERS - 1)):
                pltpu.make_async_remote_copy(
                    src_ref=row(ans, i), dst_ref=row(ret, i),
                    send_sem=rs_sem, recv_sem=rr_sem.at[j],
                    device_id=peer(i, -1), device_id_type=MESH,
                ).start()

    for j in range(PARTS):
        lo, n_rows = EDGES[j], (EDGES[j + 1] - EDGES[j]) * PAD
        with jax.named_scope(f"wait{j}"):
            landed(recv, dr_sem, j).wait()
        with jax.named_scope(f"ffn{j}"):
            x = recv[pl.ds(lo, n_rows // PAD)].reshape(n_rows, 1024)
            for n in range(4):
                g = dot(x, win[:, pl.ds(n * 256, 256)])
                t = dot(x, win[:, pl.ds(1024 + n * 256, 256)])
                act[pl.ds(0, n_rows), pl.ds(n * 256, 256)] = (g / (1.0 + jnp.exp(-g)) * t).astype(jnp.bfloat16)
            for n in range(2):
                a = dot(act[pl.ds(0, n_rows)], wout[:, pl.ds(n * 512, 512)]).astype(jnp.bfloat16)
                ans[pl.ds(lo, n_rows // PAD), :, pl.ds(n * 512, 512)] = a.reshape(n_rows // PAD, PAD, 512)
        give_back(j)
    ret[PEERS - 1] = ans[PEERS - 1]

    for n in range(4):
        loads[7 + n].wait()
    for j in range(PARTS):
        lo, n_rows = EDGES[j], (EDGES[j + 1] - EDGES[j]) * PAD
        with jax.named_scope(f"rwait{j}"):
            landed(ret, rr_sem, j).wait()
        part = dot(comb[:, pl.ds(lo * PAD, n_rows)], ret[pl.ds(lo, n_rows // PAD)].reshape(n_rows, 1024))
        if j == 0:
            head[...] = part
        elif j < PARTS - 1:
            head[...] += part
        else:
            headb[...] = (head[...] + part).astype(jnp.bfloat16)

    partner = (ys[0] + zh[0] + xs[0], zw[0] + cs[1])
    across = (ys[0] + zh[0] + xs[0], (2 - zw[0]) + cs[0])

    def send(src, dst, ss, rs, b, to):
        cols = pl.ds(*BLOCKS[b])
        return pltpu.make_async_remote_copy(
            src_ref=src.at[:, cols], dst_ref=dst.at[:, cols], send_sem=ss.at[b], recv_sem=rs.at[b],
            device_id=to, device_id_type=MESH,
        )

    def send_dd(b):
        return send(dd_s, dd_r, dd_ss, dd_rs, b, partner)

    def send_f(b):
        return send(f_s, f_r, f_ss, f_rs, b, partner)

    def send_z(b):
        return send(z_s, z_r, z_ss, z_rs, b, across)

    tops = (pl.ds(0, 128), pl.ds(128, 128))

    def product(n, b, top):
        return dot(headb[top, :], wm[n, :, pl.ds(*BLOCKS[b])])

    def first(b):
        for top in tops:
            dd_s[top, pl.ds(*BLOCKS[b])] = product(0, b, top).astype(jnp.bfloat16)
        send_dd(b).start()

    def own(b):
        for top in tops:
            head[top, pl.ds(*BLOCKS[b])] = product(1, b, top)

    def second(b):
        cols = pl.ds(*BLOCKS[b])
        send_dd(b).wait_recv()
        z_s[:, cols] = (head[:, cols] + dd_r[:, cols].astype(jnp.float32)).astype(jnp.bfloat16)
        send_z(b).start()

    blocks = range(len(BLOCKS))
    with jax.named_scope("merge"):
        first(0)
        own(0)
        first(1)
        own(1)
        second(0)
        first(2)
        second(1)
        own(2)
        first(3)
        second(2)
        own(3)
        first(4)
        second(3)
        own(4)
        second(4)
    with jax.named_scope("merge_near"):
        for b in blocks:
            for top in tops:
                f_s[top, pl.ds(*BLOCKS[b])] = product(2, b, top).astype(jnp.bfloat16)
            send_f(b).start()
        for b in range(2):
            keep[:, pl.ds(b * 512, 512)] = dot(headb[...], wm[3, :, pl.ds(b * 512, 512)])
        for b in blocks:
            cols = pl.ds(*BLOCKS[b])
            send_f(b).wait_recv()
            keep[:, cols] += f_r[:, cols].astype(jnp.float32)
        pltpu.make_async_copy(rows(packed, 0, PEERS - 1), rows(packed, 0, PEERS - 1), ds_sem).wait()
        pltpu.make_async_copy(rows(ans, 0, PEERS - 1), rows(ans, 0, PEERS - 1), rs_sem).wait()
        for b in blocks:
            send_dd(b).wait_send()
            send_f(b).wait_send()
    with jax.named_scope("final"):
        for b in blocks:
            send_z(b).wait_send()
        for b in blocks:
            send_z(b).wait_recv()


def body(tokens, w_split, w_merge, expert_in, expert_out, expert_ids, combine_q, capacity):
    bf, f32, i32 = jnp.bfloat16, jnp.float32, jnp.int32
    hbm = pl.BlockSpec(memory_space=pl.ANY)
    vm = pl.BlockSpec(memory_space=pltpu.VMEM)
    dma = pltpu.SemaphoreType.DMA
    quarter = pltpu.VMEM((256, 1024), bf)
    per_block = dma((len(BLOCKS),))
    slots = pltpu.VMEM((PEERS, PAD, 1024), bf)
    mine, other = pl.pallas_call(
        kernel,
        out_shape=[pltpu.VMEM((256, 1024), f32), pltpu.VMEM((256, 1024), bf)],
        in_specs=[hbm] * 9,
        out_specs=[vm, vm],
        scratch_shapes=[
            pltpu.VMEM((2, 256), i32),
            pltpu.VMEM((2, 256), i32),
            pltpu.VMEM((1, 128), i32),
            pltpu.VMEM((1, 128), i32),
            pltpu.VMEM((256, 4096), bf),
            pltpu.VMEM((4, 4096, 256), bf),
            pltpu.VMEM((4, 1024, 1024), bf),
            pltpu.VMEM((1024, 2048), bf),
            pltpu.VMEM((1024, 1024), bf),
            pltpu.VMEM((256, 1024), bf),
            pltpu.VMEM((1024, 256), bf),
            pltpu.VMEM((256, 1024), bf),
            slots,
            slots,
            pltpu.VMEM((max(b - a for a, b in zip(EDGES, EDGES[1:])) * PAD, 1024), bf),
            slots,
            slots,
            pltpu.VMEM((256, 1024), f32),
            pltpu.VMEM((256, 1024), bf),
            quarter, quarter, quarter, quarter, quarter,
            dma((4,)), dma((7,)), dma((4,)), dma, dma((PARTS,)), dma, dma((PARTS,)),
            per_block, per_block, per_block, per_block, per_block, per_block,
        ],
        compiler_params=pltpu.CompilerParams(
            collective_id=0, has_side_effects=True, vmem_limit_bytes=58 * 2**20
        ),
    )(
        expert_ids[0].T,
        combine_q[0].T,
        capacity.reshape(1, -1),
        jnp.asarray(POSITION).reshape(1, -1),
        tokens,
        w_split,
        w_merge,
        expert_in[0],
        expert_out[0],
    )
    return (mine + other.astype(f32)).astype(bf)


def solution(mesh):
    in_specs = (
        P("seq", None),
        P(None, "sub"),
        P("sub", None),
        P(("seq", "sub"), None, None),
        P(("seq", "sub"), None, None),
        P("sub", "seq", None),
        P("sub", "seq", None),
        P(),
    )
    return jax.shard_map(body, mesh=mesh, in_specs=in_specs, out_specs=P("seq", "sub"), check_vma=False)
```
